32 devices in a mesh: dp: 8 (over y, x, core), section: 4 (over z).
Axes of the slice: x: 2, y: 2, z: 4, core: 2. Of those that a mesh axis runs over, the one named last changes fastest.
Arguments:
- activations: bfloat16 [4, 512, 2048], P(None, 'dp'), may hold values from -6 to 6
- cotangent: bfloat16 [4, 512, 2048], P(None, 'dp'), may hold values from -6 to 6
- weight: bfloat16 [4, 2048, 2048], P('section', 'dp'), may hold values from -0.125 to 0.125
- norm_gain: float32 [4, 2048], P('section'), may hold values from 0.1 to 1.9
- pair_mask: int32 [4, 512, 2048], P('section'), may hold values from 0 to 5, as said below
- earlier_mask: int32 [4, 512, 2048], P('section', 'dp'), may hold values from 0 to 5, as said below
Outputs:
- weight_grad: float32 [4, 2048, 2048], P('section', 'dp')
- flip_count: int32 [4], P('section')
The draws below stay inside these ranges and needn't reach their ends.
Inputs may be any that keep to these rules, and one draw needn't show every extreme that they name: `pair_mask`: pair number of each group of four consecutive rows and each column; pairs numbered (0,1), (0,2), (0,3), (1,2), (1,3), (2,3). `earlier_mask`: pair numbers of the previous step, numbered likewise.
All inputs are finite; a program needn't handle non-finite values.
Results may differ from the reference program's by a relative error of at most 0.02.
Values may be sent and summed in bfloat16 or wider, within the bound.
A program may use at most 64 MiB of HBM per device.

```python
import math
import jax
import jax.numpy as jnp
from jax import lax

D = 2048
MICRO = 4
SECTIONS = 4
BATCH_ROWS = 512
TOKENS = 2048
N_DP = 8


def mask_pair(key):
    base_key = jax.random.fold_in(key, 7301)
    mask_shape = (SECTIONS, D // 4, D)
    current = jax.random.randint(jax.random.fold_in(base_key, 1), mask_shape, 0, 6)
    row_iota = lax.broadcasted_iota(jnp.int32, mask_shape, 1)
    threshold = 100 + 200 * row_iota // (D // 4 - 1)
    dice_rolls = jax.random.randint(jax.random.fold_in(base_key, 2), mask_shape, 0, 1000)
    offsets = jax.random.randint(jax.random.fold_in(base_key, 3), mask_shape, 1, 6)
    earlier = jnp.where(dice_rolls < threshold, (current + offsets) % 6, current)
    return (current.astype(jnp.int32), earlier.astype(jnp.int32))


def draw_pair_mask(key, part):
    return mask_pair(key)[0]


def draw_earlier_mask(key, part):
    return mask_pair(key)[1]


def levels(rng, shape, cuts, smallest, high):
    gain, own = 1.0, jax.random.fold_in(rng, 6)
    for position, blocks in cuts:
        steps = jnp.exp(jax.random.uniform(jax.random.fold_in(own, position), (blocks,), jnp.float32, smallest / len(cuts), high / len(cuts)))
        gain = gain * jnp.repeat(steps, shape[position] // blocks).reshape([-1 if axis == position else 1 for axis in range(len(shape))])
    return gain


def centred(key, extent, width, most, cuts=(), kind=jnp.bfloat16):
    loudness = levels(key, extent, cuts, -0.22, 0.18) if cuts else 1.0
    result = jax.random.normal(key, extent, jnp.float32) * width * loudness
    return jnp.minimum(jnp.maximum(result, -most), most).astype(kind)


def setup_inputs(seed: int = 0) -> dict:
    key_of = jax.random.split(jax.random.key(seed), 7)
    activations = centred(key_of[0], (MICRO, BATCH_ROWS, D), 1.0, 6.0, ((1, 8),))
    cotangent = centred(key_of[1], (MICRO, BATCH_ROWS, D), 1.0, 6.0, ((1, 8),))
    weight = centred(key_of[2], (SECTIONS, D, D), D ** -0.5, 0.125, ((0, 4), (1, 8)))
    norm_gain = jnp.clip(1.0 + 0.18 * jax.random.normal(key_of[3], (SECTIONS, D), jnp.float32), 0.1, 1.9)
    pair_mask = draw_pair_mask(jax.random.fold_in(key_of[6], 71), 0)
    earlier_mask = draw_earlier_mask(jax.random.fold_in(key_of[6], 71), 0)
    return {"activations": activations, "cotangent": cotangent, "weight": weight, "norm_gain": norm_gain, "pair_mask": pair_mask, "earlier_mask": earlier_mask}


epsilon = 1e-06
decay_rate = 4.0
half_root = 0.7071067811865476
density_scale = 0.3989422804014327
first_table = (0, 0, 0, 1, 1, 2)
second_table = (1, 2, 3, 2, 3, 3)

def pair_ends(indices):
    leading = jnp.zeros_like(indices)
    trailing = jnp.zeros_like(indices)
    for pair_index in range(6):
        matches = indices == pair_index
        leading = jnp.where(matches, first_table[pair_index], leading)
        trailing = jnp.where(matches, second_table[pair_index], trailing)
    return (leading, trailing)

def kept_positions(indices):
    leading, trailing = pair_ends(indices)
    groups, columns = indices.shape
    positions = lax.broadcasted_iota(jnp.int32, (groups, 4, columns), 1)
    kept_mask = (positions == leading[:, None, :]) | (positions == trailing[:, None, :])
    return kept_mask.reshape(groups * 4, columns)

def section_forward(inputs, masked, gain_row):
    values = inputs.astype(jnp.float32)
    norm_scale = lax.rsqrt(lax.optimization_barrier(jnp.mean(values * values, axis=-1, keepdims=True)) + epsilon)
    normed = (values * norm_scale * gain_row).astype(jnp.bfloat16)
    preact = jnp.dot(normed, masked, preferred_element_type=jnp.float32)
    normal_cdf = 0.5 * (1.0 + lax.erf(preact * half_root))
    outputs = (values + preact * normal_cdf).astype(jnp.bfloat16)
    return (normed, preact, outputs)

def section_backward(inputs, preact, upstream, masked, gain_row):
    values = inputs.astype(jnp.float32)
    norm_scale = lax.rsqrt(lax.optimization_barrier(jnp.mean(values * values, axis=-1, keepdims=True)) + epsilon)
    normal_cdf = 0.5 * (1.0 + lax.erf(preact * half_root))
    normal_pdf = jnp.exp(-0.5 * preact * preact) * density_scale
    upstream_f = upstream.astype(jnp.float32)
    grad_pre = (upstream_f * (normal_cdf + preact * normal_pdf)).astype(jnp.bfloat16)
    grad_normed = lax.dot_general(grad_pre, masked, (((1,), (1,)), ((), ())), preferred_element_type=jnp.float32)
    scaled_grad = grad_normed * gain_row
    grad_input = norm_scale * scaled_grad - values * norm_scale ** 3 * lax.optimization_barrier(jnp.mean(scaled_grad * values, axis=-1, keepdims=True))
    return (grad_pre, (upstream_f + grad_input).astype(jnp.bfloat16))

def replica_terms(normed, grad_pre, micro_count):
    replicas = N_DP
    model_width = normed.shape[1]
    row_count = normed.shape[0] // (micro_count * replicas)
    normed_split = normed.reshape(micro_count, replicas, row_count, model_width).transpose(1, 0, 2, 3).reshape(replicas, micro_count * row_count, model_width)
    grad_split = grad_pre.reshape(micro_count, replicas, row_count, model_width).transpose(1, 0, 2, 3).reshape(replicas, micro_count * row_count, model_width)

    def add_replica(running, pieces):
        partial_term = lax.dot_general(pieces[0], pieces[1], (((0,), (0,)), ((), ())), preferred_element_type=jnp.float32)
        rounded = lax.optimization_barrier(partial_term.astype(jnp.bfloat16))
        return (running + rounded.astype(jnp.float32), None)
    running, unused = lax.scan(add_replica, jnp.zeros((model_width, model_width), jnp.float32), (normed_split, grad_split))
    return running

def reference(activations, cotangent, weight, norm_gain, pair_mask, earlier_mask):
    micro_count, batch_rows, model_width = activations.shape
    hidden = activations.reshape(micro_count * batch_rows, model_width)
    upstream = cotangent.reshape(micro_count * batch_rows, model_width)
    masked_list = []
    kept_list = []
    for section_index in range(SECTIONS):
        kept_mask = kept_positions(pair_mask[section_index])
        kept_list.append(kept_mask)
        masked_list.append(jnp.where(kept_mask, weight[section_index], jnp.zeros_like(weight[section_index])))
    saved_inputs = []
    saved_normed = []
    saved_preact = []
    for section_index in range(SECTIONS):
        saved_inputs.append(hidden)
        normed, preact, hidden = section_forward(hidden, masked_list[section_index], norm_gain[section_index])
        saved_normed.append(normed)
        saved_preact.append(preact)
    gradients = [None] * SECTIONS
    for section_index in reversed(range(SECTIONS)):
        grad_pre, upstream = section_backward(saved_inputs[section_index], saved_preact[section_index], upstream, masked_list[section_index], norm_gain[section_index])
        dense_part = replica_terms(saved_normed[section_index], grad_pre, micro_count) / math.sqrt(TOKENS)
        decay_part = jnp.where(kept_list[section_index], 0.0, weight[section_index].astype(jnp.float32))
        gradients[section_index] = dense_part + decay_rate * decay_part
    flip_list = []
    for section_index in range(SECTIONS):
        earlier_kept = kept_positions(earlier_mask[section_index])
        flip_list.append(jnp.sum(kept_list[section_index] != earlier_kept).astype(jnp.int32))
    return (jnp.stack(gradients), jnp.stack(flip_list))
```

```python
import functools
import math

import jax
import jax.numpy as jnp
from jax import lax
from jax.experimental import pallas as pl
from jax.experimental.pallas import tpu as pltpu
from jax.sharding import PartitionSpec as P

epsilon = 1e-06
decay_rate = 4.0
half_root = 0.7071067811865476
density_scale = 0.3989422804014327
first_table = (0, 0, 0, 1, 1, 2)
second_table = (1, 2, 3, 2, 3, 3)


def shifted(block, axis, distance):
    devices = range(lax.axis_size(axis))
    route = [(i - distance, i) for i in devices if i - distance in devices]
    return lax.ppermute(block, axis, route)


def pair_ends(indices):
    leading = jnp.zeros_like(indices)
    trailing = jnp.zeros_like(indices)
    for pair_index in range(6):
        matches = indices == pair_index
        leading = jnp.where(matches, first_table[pair_index], leading)
        trailing = jnp.where(matches, second_table[pair_index], trailing)
    return (leading, trailing)


def kept_positions(indices):
    leading, trailing = pair_ends(indices)
    groups, columns = indices.shape
    positions = lax.broadcasted_iota(jnp.int32, (groups, 4, columns), 1)
    kept_mask = (positions == leading[:, None, :]) | (positions == trailing[:, None, :])
    return kept_mask.reshape(groups * 4, columns)


def section_forward(inputs, masked, gain_row):
    values = inputs.astype(jnp.float32)
    norm_scale = lax.rsqrt(jnp.mean(values * values, axis=-1, keepdims=True) + epsilon)
    normed = (values * norm_scale * gain_row).astype(jnp.bfloat16)
    preact = jnp.dot(normed, masked, preferred_element_type=jnp.float32)
    normal_cdf = 0.5 * (1.0 + lax.erf(preact * half_root))
    outputs = (values + preact * normal_cdf).astype(jnp.bfloat16)
    return (normed, preact, outputs)


def section_backward(inputs, preact, upstream, masked, gain_row):
    values = inputs.astype(jnp.float32)
    norm_scale = lax.rsqrt(jnp.mean(values * values, axis=-1, keepdims=True) + epsilon)
    normal_cdf = 0.5 * (1.0 + lax.erf(preact * half_root))
    normal_pdf = jnp.exp(-0.5 * preact * preact) * density_scale
    upstream_f = upstream.astype(jnp.float32)
    grad_pre = (upstream_f * (normal_cdf + preact * normal_pdf)).astype(jnp.bfloat16)
    grad_normed = lax.dot_general(
        grad_pre, masked, (((1,), (1,)), ((), ())), preferred_element_type=jnp.float32
    )
    scaled_grad = grad_normed * gain_row
    grad_input = norm_scale * scaled_grad - values * norm_scale**3 * jnp.mean(
        scaled_grad * values, axis=-1, keepdims=True
    )
    return (grad_pre, (upstream_f + grad_input).astype(jnp.bfloat16))


def write_slot(buffer, new_value, slot_index, is_live):
    old_value = lax.dynamic_index_in_dim(buffer, slot_index, 0, keepdims=False)
    chosen = jnp.where(is_live, new_value, old_value)
    return lax.dynamic_update_index_in_dim(buffer, chosen, slot_index, 0)


def body(activations, cotangent, weight, norm_gain, pair_mask, earlier_mask):
    section_count = lax.axis_size("section")
    replica_count = lax.axis_size("dp")
    section_index = lax.axis_index("section")
    replica_index = lax.axis_index("dp")
    micro_count, row_count, model_width = activations.shape
    shard_rows = weight.shape[1]
    groups = shard_rows // 4
    own_weight = weight[0]
    gain_row = norm_gain[0]
    own_pairs = lax.dynamic_slice_in_dim(pair_mask[0], replica_index * groups, groups, 0)
    own_kept = kept_positions(own_pairs)
    earlier_kept = kept_positions(earlier_mask[0])
    flip_local = jnp.sum(own_kept != earlier_kept).reshape(1)
    flip_sum = lax.psum(flip_local, "dp")
    masked_shard = jnp.where(own_kept, own_weight, jnp.zeros_like(own_weight))
    masked = lax.all_gather(masked_shard, "dp", axis=0, tiled=True)
    tick_count = micro_count + section_count - 1
    act_zeros = jnp.zeros((micro_count, row_count, model_width), jnp.bfloat16)
    stored = (act_zeros,)

    def forward_tick(tick_index, state_tuple):
        received, buffers = state_tuple
        micro_index = tick_index - section_index
        is_live = (micro_index >= 0) & (micro_index < micro_count)
        slot_index = jnp.clip(micro_index, 0, micro_count - 1)
        fresh_rows = lax.dynamic_index_in_dim(activations, slot_index, 0, keepdims=False)
        current = jnp.where(section_index == 0, fresh_rows, received)
        normed, preact, outputs = section_forward(current, masked, gain_row)
        results = (current, normed, preact)
        buffers = tuple(
            (
                write_slot(buffer, update, slot_index, is_live)
                for buffer, update in zip(buffers, results)
            )
        )
        received = shifted(outputs, "section", 1)
        return (received, buffers)

    start_rows = jnp.zeros((row_count, model_width), jnp.bfloat16)
    received, stored = lax.fori_loop(0, tick_count, forward_tick, (start_rows, stored))

    def backward_tick(tick_index, state_tuple):
        received, grad_buffer, normed_buffer = state_tuple
        micro_index = tick_index - (section_count - 1 - section_index)
        is_live = (micro_index >= 0) & (micro_index < micro_count)
        slot_index = jnp.clip(micro_index, 0, micro_count - 1)
        fresh_rows = lax.dynamic_index_in_dim(cotangent, slot_index, 0, keepdims=False)
        upstream = jnp.where(section_index == section_count - 1, fresh_rows, received)
        inputs = lax.dynamic_index_in_dim(stored[0], slot_index, 0, keepdims=False)
        normed, preact, unused = section_forward(inputs, masked, gain_row)
        normed_buffer = write_slot(normed_buffer, normed, slot_index, is_live)
        grad_pre, grad_input = section_backward(inputs, preact, upstream, masked, gain_row)
        grad_buffer = write_slot(grad_buffer, grad_pre, slot_index, is_live)
        received = shifted(grad_input, "section", -1)
        return (received, grad_buffer, normed_buffer)

    received, grad_buffer, normed_buffer = lax.fori_loop(
        0, tick_count, backward_tick, (start_rows, act_zeros, act_zeros)
    )
    flat_normed = normed_buffer.reshape(micro_count * row_count, model_width)
    flat_grad = grad_buffer.reshape(micro_count * row_count, model_width)
    summed = lax.psum_scatter(
        lax.dot_general(
            flat_normed, flat_grad, (((0,), (0,)), ((), ())), preferred_element_type=jnp.float32
        ).astype(jnp.bfloat16),
        "dp",
        scatter_dimension=0,
        tiled=True,
    ).astype(jnp.float32)
    token_total = micro_count * row_count * replica_count
    dense_part = summed / math.sqrt(token_total)
    decay_part = jnp.where(own_kept, 0.0, own_weight.astype(jnp.float32))
    gradient = dense_part + decay_rate * decay_part
    return (gradient[None], flip_sum)


HALVES = (0, 1)


SMALL = 16
BIG = 32
SMALL_COUNT = 4
FAR_LAG = 3
FILL = 128
LATE_ROWS = 64


def visiting_order(sizes, sections):
    arrived = [[[0.0] * len(sizes) if s == 0 and not back else [None] * len(sizes) for back in (0, 1)]
               for s in range(sections)]
    clock, link = [0.0] * sections, [[0.0, 0.0] for _ in range(sections)]
    done, masks = [[0, 0] for _ in range(sections)], [0] * sections
    while any(count < len(sizes) for pair in done for count in pair):
        choices = []
        for s in range(sections):
            ready = []
            for back in (1, 0):
                i = done[s][back]
                if i < len(sizes) and arrived[s][back][i] is not None:
                    ready.append((max(clock[s], arrived[s][back][i]), back))
            if len(ready) == 2 and ready[0][0] > ready[1][0] + 0.0:
                ready.reverse()
            if ready:
                choices.append((ready[0][0], s, ready[0][1]))
        start, s, back = min(choices)
        i = done[s][back]
        spent = 0.1 if back and s == 0 else 1.3 + 0.005 * sizes[i] + 0.15 * back
        masks[s] |= back << (done[s][0] + done[s][1])
        done[s][back] += 1
        clock[s] = start + spent + 0.06
        wire = 0.09 * sizes[i]
        link[s][back] = max(max(start + 0.45, link[s][back]) + wire, start + spent + wire / 4)
        if not back and s + 1 < sections:
            arrived[s + 1][0][i] = link[s][0] + 1.75
        if not back and s + 1 == sections:
            arrived[s][1][i] = clock[s]
        if back and s > 0:
            arrived[s - 1][1][i] = link[s][1] + 1.75
    return masks


def early_rows(rows):
    return max(rows - LATE_ROWS, SMALL * SMALL_COUNT)


def fused_fits(mesh, activations, weight):
    replicas, sections = mesh.shape["dp"], mesh.shape["section"]
    micro, batch, width = activations.shape
    shard_rows = weight.shape[1] // replicas
    rows = micro * batch // replicas
    gathered = replicas // 2 * rows * width * 2
    return (
        replicas % 2 == 0
        and replicas == 2 * len(HALVES) ** 2
        and sections > 1
        and shard_rows % 128 == 0
        and rows % BIG == 0
        and (SMALL * SMALL_COUNT) % BIG == 0
        and rows > SMALL * SMALL_COUNT + LATE_ROWS
        and 2 * (SMALL_COUNT + rows // BIG) < 30
        and width % 512 == 0
        and gathered + 5 * width * width * 2 < 56 * 2**20
    )


def spread_matrix(count, transposed):
    groups = count // 4
    rows = lax.broadcasted_iota(jnp.int32, (count, count), 1 if transposed else 0)
    columns = lax.broadcasted_iota(jnp.int32, (count, count), 0 if transposed else 1)
    place = sum((columns >= groups * j).astype(jnp.int32) for j in (1, 2, 3))
    hit = rows == 4 * (columns - groups * place) + place
    return jnp.where(hit, 1.0, 0.0).astype(jnp.bfloat16)


def fused_kernel(
    tokens, act, cot, weight, gain, pairs_hbm, earlier, own_out, sent_out, flips,
    packed, full, turned, hidden, normed, deriv, preacts, scales, outgoing, upstream, downstream, grads, terms,
    acc, partial, counts, pairs, own_pairs, load_sem, row_sem,
    pack_send, pack_recv, relay_send, relay_recv, fwd_send, fwd_recv, bwd_send, bwd_recv,
    term_send, term_recv, grad_send, pass_recv, last_recv, part_send, part_recv, flip_send, flip_recv, pair_sem, out_sem,
):
    section = lax.axis_index("section")
    sections = lax.axis_size("section")
    me = lax.axis_index("dp")
    chips = lax.axis_size("dp") // 2
    chip = lax.div(me, 2)
    core = lax.rem(me, 2)
    sibling = 2 * chip + 1 - core
    last = sections - 1
    shard_rows, width = weight.shape
    groups = shard_rows // 4
    rows = hidden.shape[0]
    steps = SMALL_COUNT + (rows - SMALL * SMALL_COUNT) // BIG
    early = early_rows(rows)
    early_steps = SMALL_COUNT + (early - SMALL * SMALL_COUNT) // BIG
    halves = (slice(0, early), slice(early, rows))
    tile = 512
    tiles = width // tile
    across = chip + 1 - 2 * lax.rem(chip, 2)
    along_y = lax.rem(chip + 2, chips)
    corner = lax.rem(across + 2, chips)
    near = (across, along_y)
    own_columns = pl.multiple_of(chip * 2 * shard_rows, 2 * shard_rows)

    def peer_chip(k):
        return lax.rem(chip + k, chips)

    def at_dp(index):
        return {"dp": index}

    def remote(src, dst, send, recv, where):
        return pltpu.make_async_remote_copy(
            src_ref=src, dst_ref=dst, send_sem=send, recv_sem=recv,
            device_id=where, device_id_type=pl.DeviceIdType.MESH,
        )

    barrier = pltpu.get_barrier_semaphore()

    def greet(where):
        pl.semaphore_signal(barrier, inc=1, device_id=where, device_id_type=pl.DeviceIdType.MESH)

    for k in range(1, chips):
        greet(at_dp(2 * peer_chip(k) + core))
    greet(at_dp(sibling))

    @pl.when(section > 0)
    def _():
        greet({"section": section - 1})

    @pl.when(section < last)
    def _():
        greet({"section": section + 1})

    own_load = pltpu.make_async_copy(
        pairs_hbm.at[pl.ds(pl.multiple_of(me * groups, groups), groups), :], own_pairs, load_sem.at[0]
    )
    own_load.start()
    all_load = pltpu.make_async_copy(pairs_hbm, pairs, load_sem.at[1])
    all_load.start()
    micro_rows = act.shape[1]

    def row_loads(source, target):
        return [
            pltpu.make_async_copy(source.at[m], target.at[pl.ds(m * micro_rows, micro_rows)], row_sem.at[m])
            for m in range(act.shape[0])
        ]

    @pl.when(section == 0)
    def _():
        for load in row_loads(act, hidden):
            load.start()

    @pl.when(section == last)
    def _():
        for load in row_loads(cot, upstream):
            load.start()

    own_load.wait()
    gather_rows = spread_matrix(shard_rows, True)
    for t in range(tiles):
        cols = slice(t * tile, (t + 1) * tile)
        split = jnp.dot(gather_rows, weight[:, cols], preferred_element_type=jnp.float32)
        w0, w1, w2, w3 = (split[j * groups:(j + 1) * groups] for j in range(4))
        p = own_pairs[:, cols]
        first = jnp.where(p <= 2, w0, jnp.where(p <= 4, w1, w2))
        second = jnp.where(p == 0, w1, jnp.where((p == 1) | (p == 3), w2, w3))
        packed[me, 0:groups, cols] = first.astype(jnp.bfloat16)
        packed[me, groups:2 * groups, cols] = second.astype(jnp.bfloat16)

    pl.semaphore_wait(barrier, chips + (section > 0).astype(jnp.int32) + (section < last).astype(jnp.int32))

    def half_rows(h):
        return pl.ds(h * groups, groups)

    def pack_copy(way, source, h, route):
        slot = packed.at[2 * source + core, half_rows(h)]
        return remote(slot, slot, pack_send.at[route, h], pack_recv.at[source, h], at_dp(2 * near[way] + core))

    def pack_own(way, h):
        return pack_copy(way, chip, h, way)

    def pack_onward(way):
        return pack_copy(1 - way, near[way], way, 2)

    def pack_arrival(source, h):
        return pack_copy(0, source, h, 0)

    def relay_copy(source, parity):
        slot = packed.at[2 * source + parity]
        return remote(slot, slot, relay_send.at[source], relay_recv.at[source], at_dp(sibling))

    for h in HALVES:
        for way in (0, 1):
            pack_own(way, h if way == 0 else 1 - h).start()
    relay_copy(chip, core).start()

    p = own_pairs[...]
    q = earlier[...]
    changed = jnp.where(p == q, 0, jnp.where(p + q == 5, 4, 2))
    total = jnp.zeros((8, 128), jnp.int32)
    for a in range(groups // 8):
        for b in range(width // 128):
            total = total + changed[a * 8:(a + 1) * 8, b * 128:(b + 1) * 128]
    counts[chip] = total

    def flip_copy(k, source):
        slot = counts.at[source]
        return remote(slot, slot, flip_send.at[k], flip_recv.at[source], at_dp(2 * peer_chip(k) + core))

    for k in range(1, chips):
        flip_copy(k, chip).start()

    spread_rows = spread_matrix(shard_rows, False)

    def unpack(owner):
        owned = pl.multiple_of(owner * groups, groups)
        target = pl.multiple_of(owner * shard_rows, shard_rows)
        for t in range(tiles):
            cols = slice(t * tile, (t + 1) * tile)
            p = pairs[pl.ds(owned, groups), cols]
            v0 = packed[owner, 0:groups, cols].astype(jnp.float32)
            v1 = packed[owner, groups:2 * groups, cols].astype(jnp.float32)
            zero = jnp.zeros_like(v0)
            parts = (
                jnp.where(p <= 2, v0, zero),
                jnp.where((p == 3) | (p == 4), v0, jnp.where(p == 0, v1, zero)),
                jnp.where(p == 5, v0, jnp.where((p == 1) | (p == 3), v1, zero)),
                jnp.where((p == 2) | (p >= 4), v1, zero),
            )
            stacked = jnp.concatenate(parts, axis=0).astype(jnp.bfloat16)
            spread = jnp.dot(spread_rows, stacked, preferred_element_type=jnp.float32)
            full[pl.ds(target, shard_rows), cols] = spread.astype(jnp.bfloat16)

    all_load.wait()

    block = 256
    same = lax.broadcasted_iota(jnp.int32, (block, block), 0) == lax.broadcasted_iota(jnp.int32, (block, block), 1)
    unit = jnp.where(same, 1.0, 0.0).astype(jnp.bfloat16)

    def turn(first_owner):
        source = pl.ds(pl.multiple_of(first_owner * shard_rows, 2 * shard_rows), 2 * shard_rows)
        for b in range(width // block):
            cols = slice(b * block, (b + 1) * block)
            flipped = lax.dot_general(
                unit, full[source, cols], (((1,), (1,)), ((), ())), preferred_element_type=jnp.float32
            )
            turned[cols, source] = flipped.astype(jnp.bfloat16)

    def unpack_two(first, second):
        def one(k, carry):
            unpack(jnp.where(k == 0, first, second))
            return carry

        lax.fori_loop(0, 2, one, 0)

    def turn_some(*owners):
        @pl.when(section > 0)
        def _():
            def one(k, carry):
                owner = jnp.int32(owners[0])
                for n in range(1, len(owners)):
                    owner = jnp.where(k == n, owners[n], owner)
                turn(owner)
                return carry

            lax.fori_loop(0, len(owners), one, 0)

    relay_copy(chip, 1 - core).wait_recv()
    unpack_two(2 * chip + core, 2 * chip + 1 - core)
    turn_some(2 * chip)
    for way in (0, 1):
        pack_arrival(near[way], way).wait_recv()
        pack_onward(way).start()
    for way in (0, 1):
        pack_arrival(near[way], 1 - way).wait_recv()
        relay_copy(near[way], core).start()
    unpack_two(2 * across + core, 2 * along_y + core)
    for way in (0, 1):
        relay_copy(near[way], 1 - core).wait_recv()
    unpack_two(2 * across + 1 - core, 2 * along_y + 1 - core)
    turn_some(2 * across, 2 * along_y)
    for h in HALVES:
        pack_arrival(corner, h).wait_recv()
    relay_copy(corner, core).start()
    unpack_two_first = 2 * corner + core
    relay_copy(corner, 1 - core).wait_recv()
    unpack_two(unpack_two_first, 2 * corner + 1 - core)
    turn_some(2 * corner)

    @pl.when(section == 0)
    def _():
        for load in row_loads(act, hidden):
            load.wait()

    @pl.when(section == last)
    def _():
        for load in row_loads(cot, upstream):
            load.wait()

    def span(i, size):
        if size == SMALL:
            return pl.ds(pl.multiple_of(i * SMALL, SMALL), size)
        return pl.ds(pl.multiple_of(SMALL * SMALL_COUNT + (i - SMALL_COUNT) * BIG, BIG), size)

    def fwd_copy(where, cols, i, to):
        return remote(outgoing.at[where, cols], hidden.at[where, cols], fwd_send, fwd_recv.at[i], {"section": to})

    def bwd_copy(where, cols, i, to):
        return remote(downstream.at[where, cols], upstream.at[where, cols], bwd_send, bwd_recv.at[i], {"section": to})

    everything = slice(0, width)

    def part_of(i):
        return jnp.where(i >= early_steps, 1, 0)

    def term_copy(k, where, part):
        peer = peer_chip(k)
        wanted = pl.ds(pl.multiple_of(peer * 2 * shard_rows, 2 * shard_rows), 2 * shard_rows)
        return remote(
            normed.at[where, wanted], terms.at[chip, where],
            term_send.at[k], term_recv.at[chip, part], at_dp(2 * peer + core),
        )

    def half_columns(h):
        return pl.ds(h * (width // 2), width // 2)

    def grad_passed(way, source, where, i):
        slot = grads.at[source, where, half_columns(way)]
        return remote(slot, slot, grad_send.at[way, 0], pass_recv.at[way, i], at_dp(2 * near[way] + core))

    def grad_final(way, source, h, route, where, part):
        slot = grads.at[source, where, half_columns(h)]
        return remote(
            slot, slot, grad_send.at[way, route], last_recv.at[source * 2 + h, part], at_dp(2 * near[way] + core)
        )

    def grad_onward(way, where, part):
        return grad_final(1 - way, near[way], way, 2, where, part)

    def pass_on(i, size):
        where = span(i, size)
        for way in (0, 1):
            grad_passed(way, near[way], where, i).wait_recv()
            grad_onward(way, where, part_of(i)).start()

    def filled(block):
        if block.shape[0] <= SMALL:
            return block
        return jnp.concatenate([block] * (FILL // block.shape[0]), axis=0)

    def forward(i, size, sends):
        where = span(i, size)

        @pl.when(section > 0)
        def _():
            fwd_copy(where, everything, i, section).wait_recv()

        values = hidden[where].astype(jnp.float32)
        lifted = values * gain[...]
        ready = lifted.astype(jnp.bfloat16)
        scale = lax.rsqrt(jnp.mean(values * values, axis=-1, keepdims=True) + epsilon)
        scales[where] = jnp.broadcast_to(scale, (size, 128))
        column_tiles = [slice(t * tile, (t + 1) * tile) for t in range(tiles)]

        streamed = filled(ready)

        def multiply(cols):
            return jnp.dot(streamed, full[:, cols], preferred_element_type=jnp.float32)[:size]

        later = multiply(column_tiles[0])
        for t, cols in enumerate(column_tiles):
            preact = scale * later
            if t + 1 < tiles:
                later = multiply(column_tiles[t + 1])
            cdf = 0.5 * (1.0 + lax.erf(preact * half_root))
            pdf = jnp.exp(-0.5 * preact * preact) * density_scale
            preacts[where, cols] = preact
            deriv[where, cols] = cdf + preact * pdf
            if sends:
                outgoing[where, cols] = (values[:, cols] + preact * cdf).astype(jnp.bfloat16)
                fwd_copy(where, cols, i, section + 1).start()
        normed[where] = (lifted * scale).astype(jnp.bfloat16)
        terms[chip, where] = normed[where, pl.ds(own_columns, 2 * shard_rows)]
        for k in range(1, chips):
            term_copy(k, where, part_of(i)).start()

    def backward(i, size, sends):
        where = span(i, size)

        @pl.when(section < last)
        def _():
            bwd_copy(where, everything, i, section).wait_recv()

        above = upstream[where].astype(jnp.float32)
        slope = above * deriv[where]
        grad_pre = slope.astype(jnp.bfloat16)
        grads[chip, where] = grad_pre
        if sends:
            scale = scales[where, 0:1]
            along = jnp.sum(slope * preacts[where], axis=-1, keepdims=True)
            pull = scale * scale * (along / width)
            column_tiles = [slice(t * tile, (t + 1) * tile) for t in range(tiles)]

            streamed = filled(grad_pre)

            def multiply(cols):
                return jnp.dot(streamed, turned[:, cols], preferred_element_type=jnp.float32)[:size]

            later = multiply(column_tiles[0])
            for t, cols in enumerate(column_tiles):
                piece = later * gain[:, cols]
                if t + 1 < tiles:
                    later = multiply(column_tiles[t + 1])
                result = (
                    upstream[where, cols].astype(jnp.float32)
                    + scale * piece
                    - hidden[where, cols].astype(jnp.float32) * pull
                )
                downstream[where, cols] = result.astype(jnp.bfloat16)
                bwd_copy(where, cols, i, section - 1).start()
        for way in (0, 1):
            grad_passed(way, chip, where, i).start()
        for way in (0, 1):
            grad_final(way, chip, 1 - way, 1, where, part_of(i)).start()

    def by_size(i, action):
        @pl.when(i < SMALL_COUNT)
        def _():
            action(i, SMALL)

        @pl.when(i >= SMALL_COUNT)
        def _():
            action(i, BIG)

    lag = jnp.where(section == 0, 1, min(FAR_LAG, steps - SMALL_COUNT))
    sizes = [SMALL] * SMALL_COUNT + [BIG] * (steps - SMALL_COUNT)
    order = jnp.int32(0)
    for s, mask in enumerate(visiting_order(sizes, sections)):
        order = jnp.where(section == s, mask, order)

    def step(k, carry):
        left, forwards = carry
        back_bit = lax.rem(left, 2)
        goes_back = back_bit == 1
        index = jnp.where(goes_back, k - forwards, forwards)

        @pl.when(jnp.logical_not(goes_back) & (section < last))
        def _():
            by_size(index, lambda i, size: forward(i, size, True))

        @pl.when(jnp.logical_not(goes_back) & (section == last))
        def _():
            by_size(index, lambda i, size: forward(i, size, False))

        @pl.when(goes_back & (section > 0))
        def _():
            by_size(index, lambda i, size: backward(i, size, True))

        @pl.when(goes_back & (section == 0))
        def _():
            by_size(index, lambda i, size: backward(i, size, False))

        @pl.when(goes_back & (index >= lag))
        def _():
            by_size(index - lag, pass_on)

        return lax.div(left, 2), forwards + 1 - back_bit

    lax.fori_loop(0, 2 * steps, step, (order, jnp.int32(0)))

    def arrivals(part):
        where = halves[part]
        for k in range(1, chips):
            source = peer_chip(k)
            slot = terms.at[source, where]
            remote(slot, slot, term_send.at[k], term_recv.at[source, part], at_dp(2 * peer_chip(k) + core)).wait_recv()
        for way in (0, 1):
            grad_final(way, near[way], 1 - way, 1, where, part).wait_recv()
        for h in HALVES:
            grad_final(0, corner, h, 2, where, part).wait_recv()

    def product(half, cols, part):
        left = pl.ds(pl.multiple_of(half * shard_rows, shard_rows), shard_rows)
        rows_of = halves[part]
        total = jnp.zeros((shard_rows, tile), jnp.float32)
        if part == 0:
            for c in range(chips):
                total = total + lax.dot_general(
                    terms[c, rows_of, left], grads[c, rows_of, cols],
                    (((0,), (0,)), ((), ())), preferred_element_type=jnp.float32,
                )
            return total
        stacked = [jnp.concatenate([ref[c, rows_of, which] for c in range(chips)], axis=0)
                   for ref, which in ((terms, left), (grads, cols))]
        return lax.dot_general(
            stacked[0], stacked[1], (((0,), (0,)), ((), ())), preferred_element_type=jnp.float32
        )

    def pass_rest(i, carry):
        pass_on(i, BIG)
        return carry

    for k in range(1, chips):
        flip_copy(k, peer_chip(k)).wait_recv()
    total = counts[0]
    for c in range(1, chips):
        total = total + counts[c]
    counts[chips] = total
    pair_copy = remote(counts.at[chips], counts.at[chips + 1], pair_sem.at[0], pair_sem.at[1], at_dp(sibling))
    pair_copy.start()
    lax.fori_loop(steps - lag, steps, pass_rest, 0)
    pair_copy.wait()
    flips[0] = jnp.sum(counts[chips] + counts[chips + 1])
    arrivals(0)
    for t in range(tiles):
        cols = slice(t * tile, (t + 1) * tile)
        for side in (0, 1):
            acc[side, :, cols] = product(jnp.where(side == 0, 1 - core, core), cols, 0)
    arrivals(1)

    def part_copy(t):
        return remote(
            partial.at[t], sent_out.at[:, pl.ds(t * tile, tile)], part_send, part_recv, at_dp(sibling)
        )

    def own_copy(t):
        cols = pl.ds(t * tile, tile)
        return pltpu.make_async_copy(acc.at[1, :, cols], own_out.at[:, cols], out_sem.at[t])

    for t in range(tiles):
        cols = slice(t * tile, (t + 1) * tile)
        partial[t] = (acc[0, :, cols] + product(1 - core, cols, 1)).astype(jnp.bfloat16)
        part_copy(t).start()
    own_rows = pl.ds(pl.multiple_of(me * shard_rows, shard_rows), shard_rows)
    for t in range(tiles):
        cols = slice(t * tile, (t + 1) * tile)
        pruned = weight[:, cols].astype(jnp.float32) - full[own_rows, cols].astype(jnp.float32)
        dense = acc[1, :, cols] + product(core, cols, 1)
        acc[1, :, cols] = dense * (1.0 / math.sqrt(tokens)) + decay_rate * pruned
        own_copy(t).start()

    everything_sent = remote(partial, partial, part_send, part_recv, at_dp(sibling))
    for t in range(tiles):
        own_copy(t).wait()
    everything_sent.wait_recv()
    everything_sent.wait_send()
    for k in range(1, chips):
        flip_copy(k, chip).wait_send()

    for way in (0, 1):
        pack_onward(way).wait_send()
        for h in HALVES:
            pack_own(way, h).wait_send()
    for c in range(chips):
        relay_copy(c, core).wait_send()

    whole = slice(0, rows)
    for k in range(1, chips):
        term_copy(k, whole, 0).wait_send()
    for way in (0, 1):
        slot = grads.at[chip, whole, half_columns(way)]
        for route in (0, 1, 2):
            remote(
                slot, slot, grad_send.at[way, route], last_recv.at[0, 0], at_dp(2 * near[way] + core)
            ).wait_send()

    @pl.when(section < last)
    def _():
        fwd_copy(whole, everything, 0, section + 1).wait_send()

    @pl.when(section > 0)
    def _():
        bwd_copy(whole, everything, 0, section - 1).wait_send()


def fused_body(activations, cotangent, weight, norm_gain, pair_mask, earlier_mask):
    replicas = lax.axis_size("dp")
    chips = replicas // 2
    micro, micro_rows, width = activations.shape
    shard_rows = weight.shape[1]
    groups = shard_rows // 4
    rows = micro * micro_rows
    steps = SMALL_COUNT + (rows - SMALL * SMALL_COUNT) // BIG
    tile = 512
    tiles = width // tile
    bf, f32 = jnp.bfloat16, jnp.float32
    dma = pltpu.SemaphoreType.DMA
    vmem = pl.BlockSpec(memory_space=pltpu.VMEM)
    hbm = pl.BlockSpec(memory_space=pl.ANY)
    own, sent, flips = pl.pallas_call(
        functools.partial(fused_kernel, rows * replicas),
        out_shape=(
            jax.ShapeDtypeStruct((shard_rows, width), f32),
            jax.ShapeDtypeStruct((shard_rows, width), bf),
            jax.ShapeDtypeStruct((1,), jnp.int32),
        ),
        in_specs=[hbm, hbm, vmem, vmem, hbm, vmem],
        out_specs=(hbm, hbm, pl.BlockSpec(memory_space=pltpu.SMEM)),
        scratch_shapes=[
            pltpu.VMEM((replicas, 2 * groups, width), bf),
            pltpu.VMEM((width, width), bf),
            pltpu.VMEM((width, width), bf),
            pltpu.VMEM((rows, width), bf),
            pltpu.VMEM((rows, width), bf),
            pltpu.VMEM((rows, width), f32),
            pltpu.VMEM((rows, width), f32),
            pltpu.VMEM((rows, 128), f32),
            pltpu.VMEM((rows, width), bf),
            pltpu.VMEM((rows, width), bf),
            pltpu.VMEM((rows, width), bf),
            pltpu.VMEM((chips, rows, width), bf),
            pltpu.VMEM((chips, rows, 2 * shard_rows), bf),
            pltpu.VMEM((2, shard_rows, width), f32),
            pltpu.VMEM((tiles, shard_rows, tile), bf),
            pltpu.VMEM((chips + 2, 8, 128), jnp.int32),
            pltpu.VMEM((width // 4, width), jnp.int32),
            pltpu.VMEM((groups, width), jnp.int32),
            dma((2,)), dma((micro,)),
            dma((3, 2)), dma((chips, 2)), dma((chips,)), dma((chips,)),
            dma, dma((steps,)), dma, dma((steps,)),
            dma((chips,)), dma((chips, 2)), dma((2, 3)), dma((2, steps)), dma((2 * chips, 2)),
            dma, dma, dma((chips,)), dma((chips,)), dma((2,)), dma((tiles,)),
        ],
        compiler_params=pltpu.CompilerParams(
            collective_id=0, has_side_effects=True, vmem_limit_bytes=60 * 2**20
        ),
        name="fused_step",
    )(
        activations, cotangent, weight[0], norm_gain, pair_mask[0], earlier_mask[0],
    )
    gradient = own + sent.astype(f32) * (1.0 / math.sqrt(rows * replicas))
    return (gradient[None], flips)


def solution(mesh):
    placed = (
        P(None, "dp", None),
        P(None, "dp", None),
        P("section", "dp", None),
        P("section", None),
        P("section", None, None),
        P("section", "dp", None),
    )

    def step(*arrays):
        chosen = fused_body if fused_fits(mesh, arrays[0], arrays[2]) else body
        return jax.shard_map(
            chosen,
            mesh=mesh,
            in_specs=placed,
            out_specs=(P("section", "dp", None), P("section")),
            check_vma=False,
        )(*arrays)

    return step
```
